128 devices in a mesh: dp: 16 (over x, z_lo, core), tensor: 8 (over y, z_hi).
Axes of the slice: x: 4, y: 4, z: 4 (z_hi: 2, z_lo: 2; z = z_hi * 2 + z_lo), core: 2. Of those that a mesh axis runs over, the one named last changes fastest.
Arguments:
- acts: bfloat16 [16384, 3584], P('dp'), may hold values from -6 to 6
- cotangent: bfloat16 [16384, 18944], P('dp', 'tensor'), may hold values from -6 to 6
- hessian_ema: float32 [3584, 18944], P('dp', 'tensor'), may hold values from 0.02 to 2
- momentum: float32 [3584, 18944], P('dp', 'tensor'), may hold values from -0.12 to 0.12
- gamma_table: float32 [28], replicated, may hold values from 0.005 to 0.02
- layer_index: int32 [1], replicated, may hold values from 0 to 27
- step_count: int32 [1], replicated, may hold values from 1 to 20
Outputs:
- new_hessian: float32 [67895296], P(('dp', 'tensor'))
- ratio: float32 [67895296], P(('dp', 'tensor'))
The draws below stay inside these ranges and needn't reach their ends.
All inputs are finite; a program needn't handle non-finite values.
Results may differ from the reference program's by a relative error of at most 0.0003.
Values sent between devices are 32-bit elements; how exact they have to be, the bound alone decides.
A program may use at most 128 MiB of HBM per device.

```python
import math
import jax
import jax.numpy as jnp
from jax import lax

D = 3584
FF = 18944
LAYERS_ALL = 28
TOKENS = 16384


def raised(array, rng, source, target, parts, factor):
    def block_of(axis_at):
        return (jnp.arange(array.shape[axis_at]) // (array.shape[axis_at] // parts)).reshape((-1,) + (1,) * (array.ndim - 1 - axis_at))

    one_side = jax.random.permutation(rng, parts)[block_of(target)]
    far = (block_of(target) + parts // 2) % parts
    return jnp.where((block_of(source) == one_side) | (block_of(source) == far), factor * array, array)


def block_scale(rng, shape, pieces, least, top_value):
    loudness = 1.0
    for axis_at, shards_of in pieces:
        draws = jax.random.uniform(jax.random.fold_in(jax.random.fold_in(rng, 6), axis_at), (shards_of,), jnp.float32, least / len(pieces), top_value / len(pieces))
        loudness = loudness * jnp.repeat(jnp.exp(draws), shape[axis_at] // shards_of).reshape((-1,) + (1,) * (len(shape) - 1 - axis_at))
    return loudness


def normal_values(own_key, dims, deviation, limit, shards=(), kind=jnp.bfloat16):
    array = deviation * jax.random.normal(own_key, dims, jnp.float32)
    if shards:
        array = array * block_scale(own_key, dims, shards, -0.22, 0.18)
    return jnp.clip(array, -limit, limit).astype(kind)


def gaussian_with(stream_key, extent, spread, reach, pieces, heavy, kind=jnp.bfloat16):
    values = spread * jax.random.normal(stream_key, extent, jnp.float32)
    if pieces:
        values = values * block_scale(stream_key, extent, pieces, -0.22, 0.18)
    return jnp.clip(raised(values, jax.random.fold_in(stream_key, 3), *heavy), -reach, reach).astype(kind)


def setup_inputs(seed: int = 0) -> dict:
    key_list = jax.random.split(jax.random.key(seed), 8)
    acts = gaussian_with(key_list[0], (TOKENS, D), 1.0, 6.0, ((0, 16),), (0, 1, 16, 2.0))
    cotangent = normal_values(key_list[1], (TOKENS, FF), 1.0, 6.0, ((0, 16), (1, 8)))
    hessian_ema = jnp.clip(jnp.exp(math.log(2.0) - 4.6051702 * jax.random.uniform(key_list[2], (D, FF), jnp.float32) ** block_scale(key_list[2], (D, FF), ((0, 16), (1, 8)), -0.2, 0.2)), 0.02, 2.0)
    momentum = normal_values(key_list[3], (D, FF), 0.02, 0.12, ((0, 16), (1, 8)), jnp.float32)
    gamma_table = jnp.clip(jnp.exp(jax.random.uniform(key_list[4], (LAYERS_ALL,), jnp.float32, math.log(0.005), math.log(0.02))), 0.005, 0.02)
    layer_index = jax.random.randint(key_list[5], (1,), 0, LAYERS_ALL).astype(jnp.int32)
    step_count = jax.random.randint(key_list[6], (1,), 1, 21).astype(jnp.int32)
    return {"acts": acts, "cotangent": cotangent, "hessian_ema": hessian_ema, "momentum": momentum, "gamma_table": gamma_table, "layer_index": layer_index, "step_count": step_count}


def reference(acts, cotangent, hessian_ema, momentum, gamma_table, layer_index, step_count):
    grad_sum = lax.dot_general(acts, cotangent, (((0,), (0,)), ((), ())), preferred_element_type=jnp.float32)
    estimate = grad_sum * grad_sum / float(TOKENS)
    fresh = 0.99 * hessian_ema + 0.01 * estimate
    picks = jnp.arange(LAYERS_ALL, dtype=jnp.int32) == layer_index[0]
    gamma = jnp.sum(jnp.where(picks, gamma_table, jnp.zeros_like(gamma_table)))
    correction = 1.0 - jnp.power(jnp.asarray(0.99, gamma_table.dtype), step_count[0].astype(gamma_table.dtype))
    corrected = fresh / correction
    ratio = jnp.clip(momentum / (gamma * corrected), -1.0, 1.0)
    return fresh.reshape(-1), ratio.reshape(-1)
```

```python
import jax
import jax.numpy as jnp
from jax import lax
from jax.experimental import pallas as pl
from jax.experimental.pallas import tpu as pltpu
from jax.sharding import PartitionSpec as P

TOKENS = 16384
MESH = pl.DeviceIdType.MESH
LANES = 128
WIN = 32

NT = 19
NS = 4
ND = 3
NQ = 3


def kernel(acts, cot_t, hess, mom, gamma_table, layer, steps, fresh_out, ratio_out,
           acts_t, stage, cot, h_in, m_in, tail,
           d_send, d_recv, s_buf, far, direct, relay, q_buf, z_recv, a_send, g_buf, hm_send, hm_buf,
           fresh, ratio,
           ld_sem, cot_sem, st_sem,
           d_ssem, d_rsem, d_free, x_ssem, far_sem, direct_sem, relay_sem,
           z_ssem, z_rsem, a_ssem, a_rsem, h_ssem, h_rsem, o_sem):
    dp = lax.axis_index("dp")
    tn = lax.axis_index("tensor")
    core = lax.rem(dp, 2)
    m = lax.rem(lax.div(dp, 2), 2)
    x = lax.div(dp, 4)
    h = lax.rem(tn, 2)
    y = lax.div(tn, 2)

    def dp_of(x_, m_, core_):
        return (x_ * 2 + m_) * 2 + core_

    partner = (dp_of(x, m, 1 - core), tn)
    right = (dp_of(lax.rem(x + 1, 4), m, core), tn)
    left = (dp_of(lax.rem(x + 3, 4), m, core), tn)
    zpeer = (dp_of(x, 1 - m, core), tn)
    flip_dp = dp_of(x, 1 - m, core)

    acts_ld = [pltpu.make_async_copy(acts.at[:, pl.ds(p * 896, 896)], stage.at[p % 2], ld_sem.at[p]) for p in range(4)]
    acts_ld[0].start()
    acts_ld[1].start()
    cot_ld = [
        pltpu.make_async_copy(cot_t.at[pl.ds(lo, n)], cot.at[pl.ds(pl.multiple_of(lo + 64 * h, 64), n)], cot_sem.at[k])
        for k, (lo, n) in enumerate(((0, 256), (256, 2112)))
    ]
    cot_ld[0].start()
    cot_ld[1].start()
    st_ld = [pltpu.make_async_copy(hess, h_in, st_sem.at[0]), pltpu.make_async_copy(mom, m_in, st_sem.at[1])]
    st_ld[0].start()
    st_ld[1].start()

    barrier = pltpu.get_barrier_semaphore()
    peers = [partner, right, left, zpeer]
    for k in range(1, 8):
        peers.append((dp, lax.rem(tn + k, 8)))
    for k in range(4):
        peers.append((flip_dp, k * 2 + 1 - h))
    for peer in peers:
        pl.semaphore_signal(barrier, inc=1, device_id=peer, device_id_type=MESH)

    cot[pl.ds(pl.multiple_of((1 - h) * 2368, 64), 64), :] = jnp.zeros((64, 1024), jnp.bfloat16)

    for p in range(4):
        acts_ld[p].wait()
        for k in range(7):
            block = stage[p % 2, :, k * LANES:(k + 1) * LANES].T
            row = k * LANES
            done = 0
            while done < LANES:
                which, inside = divmod(row + done, 224)
                size = min(224 - inside, LANES - done)
                dest = (2 * p + which // 2) * 224 + inside
                acts_t[which % 2, dest:dest + size, :] = block[done:done + size]
                done += size
        if p + 2 < 4:
            acts_ld[p + 2].start()
    cot_ld[0].wait()
    cot_ld[1].wait()
    st_ld[0].wait()
    st_ld[1].wait()
    for k, ref in enumerate((h_in, m_in)):
        tail[k] = jnp.concatenate([ref[:, 2304:], jnp.zeros((224, 64), jnp.float32)], axis=1)

    pl.semaphore_wait(barrier, len(peers))

    def product(which, n):
        return lax.dot_general(
            acts_t[which], cot[pl.ds(pl.multiple_of(n * LANES, LANES), LANES), :],
            (((1,), (1,)), ((), ())), preferred_element_type=jnp.float32)

    def remote(src, dst, ssem, rsem, dev):
        return pltpu.make_async_remote_copy(src_ref=src, dst_ref=dst, send_sem=ssem, recv_sem=rsem,
                                            device_id=dev, device_id_type=MESH)

    def d_copy(n):
        return remote(d_send.at[lax.rem(n, 2)], d_recv.at[lax.rem(n, ND)], d_ssem.at[lax.rem(n, 2)],
                      d_rsem.at[lax.rem(n, ND)], partner)

    def blk(n, x_, m_):
        return s_buf.at[lax.rem(n, NS), lax.rem(x + x_, 4) * 2 + m_]

    def x_copies(n):
        s = lax.rem(n, NS)
        return (
            remote(blk(n, 2, 0), far.at[n, 0], x_ssem.at[s, 0], far_sem.at[n, 0], left),
            remote(blk(n, 2, 1), far.at[n, 1], x_ssem.at[s, 1], far_sem.at[n, 1], right),
            remote(blk(n, 1, 0), direct.at[n, 0], x_ssem.at[s, 2], direct_sem.at[n, 0], right),
            remote(blk(n, 3, 1), direct.at[n, 1], x_ssem.at[s, 3], direct_sem.at[n, 1], left),
            remote(blk(n, 3, 0), relay.at[n, 0], x_ssem.at[s, 4], relay_sem.at[n, 0], left),
            remote(blk(n, 1, 1), relay.at[n, 1], x_ssem.at[s, 5], relay_sem.at[n, 1], right),
        )

    def z_copies(n):
        s = lax.rem(n, NQ)
        return (
            remote(q_buf.at[s, 1 - m, :, pl.ds(pl.multiple_of(24 * h, 8), WIN), :], z_recv.at[n, 0],
                   z_ssem.at[s, 0], z_rsem.at[n, 0], zpeer),
            remote(q_buf.at[s, m, :, pl.ds(pl.multiple_of(24 * (1 - h), 8), WIN), :], z_recv.at[n, 1],
                   z_ssem.at[s, 1], z_rsem.at[n, 1], zpeer),
        )

    def a_copies(n):
        s = lax.rem(n, NQ)
        out = []
        for k in range(1, 4):
            to = lax.rem(y + k, 4)
            out.append(remote(a_send.at[s, 0, to], g_buf.at[tn, n], a_ssem.at[s, k - 1], a_rsem.at[n], (dp, to * 2 + h)))
        for k in range(4):
            to = lax.rem(y + k, 4)
            out.append(remote(a_send.at[s, 1, to], g_buf.at[tn, n], a_ssem.at[s, 3 + k], a_rsem.at[n], (flip_dp, to * 2 + 1 - h)))
        return out

    def h_copies(n):
        s = lax.rem(n, NQ)
        out = []
        for k in range(1, 8):
            to = lax.rem(tn + k, 8)
            out.append(remote(hm_send.at[s, :, lax.div(to, 2), pl.ds(pl.multiple_of(24 * lax.rem(to, 2), 8), WIN), :],
                              hm_buf.at[tn, n], h_ssem.at[s, k - 1], h_rsem.at[n], (dp, to)))
        return out

    correction_power = jnp.float32(1.0)
    count = steps[0]
    for bit in range(15):
        correction_power = jnp.where(lax.rem(lax.div(count, 2 ** bit), 2) == 1,
                                     correction_power * jnp.float32(0.99 ** (2 ** bit)), correction_power)
    correction = 1.0 - correction_power
    factor = correction / gamma_table[layer[0]]

    def finish(tile, g, hs, mo):
        new = 0.99 * hs + (0.01 / TOKENS) * (g * g)
        fresh[pl.ds(tile, WIN, stride=148), :] = new
        ratio[pl.ds(tile, WIN, stride=148), :] = jnp.clip(mo * factor / new, -1.0, 1.0)

    lane = lax.broadcasted_iota(jnp.int32, (224, LANES), 1)

    def state_tile(k, ref, n):
        at = lambda i: ref[:, pl.ds(pl.multiple_of(i * LANES, LANES), LANES)]
        here = jnp.where(n < NT - 1, at(jnp.minimum(n, NT - 2)), tail[k])
        before = jnp.where(n > 0, at(jnp.maximum(n - 1, 0)), 0.0)
        moved = jnp.where(lane < 64, pltpu.roll(before, 64, 1), pltpu.roll(here, 64, 1))
        return jnp.where(h == 0, here, moved)

    def body(t, carry):
        n = t

        @pl.when(n < NT)
        def _():
            s = lax.rem(n, NQ)

            @pl.when(n >= NQ)
            def _():
                for c in h_copies(n - NQ):
                    c.wait_send()
            hm_send[s, 0] = state_tile(0, h_in, n).reshape(4, 56, LANES)
            hm_send[s, 1] = state_tile(1, m_in, n).reshape(4, 56, LANES)
            hm_buf[tn, n] = hm_send[s, :, y, pl.ds(pl.multiple_of(24 * h, 8), WIN), :]
            for c in h_copies(n):
                c.start()

            @pl.when(n >= 2)
            def _():
                d_copy(n - 2).wait_send()
            d_send[lax.rem(n, 2)] = product(1 - core, n)

            @pl.when(n >= ND)
            def _():
                pl.semaphore_wait(d_free, 1)
            d_copy(n).start()

        n1 = t - 1

        @pl.when(jnp.logical_and(n1 >= 0, n1 < NT))
        def _():
            @pl.when(n1 >= NS)
            def _():
                for c in x_copies(n1 - NS):
                    c.wait_send()
            own = product(core, n1)
            d_copy(n1).wait_recv()
            s_buf[lax.rem(n1, NS)] = (own + d_recv[lax.rem(n1, ND)]).reshape(8, 224, LANES)

            @pl.when(n1 < NT - ND)
            def _():
                pl.semaphore_signal(d_free, inc=1, device_id=partner, device_id_type=MESH)
            for c in x_copies(n1)[:4]:
                c.start()

        n2 = t - 2

        @pl.when(jnp.logical_and(n2 >= 0, n2 < NT))
        def _():
            cs = x_copies(n2)
            for half, c, at in ((0, cs[4], 3), (1, cs[5], 1)):
                cs[half].wait_recv()
                b = blk(n2, at, half)
                b[...] = b[...] + far[n2, half]
                c.start()

        n3 = t - 3

        @pl.when(jnp.logical_and(n3 >= 0, n3 < NT))
        def _():
            @pl.when(n3 >= NQ)
            def _():
                for c in z_copies(n3 - NQ):
                    c.wait_send()
            cs = x_copies(n3)
            for half in range(2):
                cs[2 + half].wait_recv()
                cs[4 + half].wait_recv()
                total = blk(n3, 0, half)[...] + direct[n3, half] + relay[n3, half]
                q_buf[lax.rem(n3, NQ), half] = total.reshape(4, 56, LANES)
            for c in z_copies(n3):
                c.start()

        n4 = t - 4

        @pl.when(jnp.logical_and(n4 >= 0, n4 < NT))
        def _():
            s = lax.rem(n4, NQ)

            @pl.when(n4 >= NQ)
            def _():
                for c in a_copies(n4 - NQ):
                    c.wait_send()
            for c in z_copies(n4):
                c.wait_recv()
            a_send[s, 0] = q_buf[s, m, :, pl.ds(pl.multiple_of(24 * h, 8), WIN), :] + z_recv[n4, 0]
            a_send[s, 1] = q_buf[s, 1 - m, :, pl.ds(pl.multiple_of(24 * (1 - h), 8), WIN), :] + z_recv[n4, 1]
            g_buf[tn, n4] = a_send[s, 0, y]
            for c in a_copies(n4):
                c.start()

        n5 = t - 5

        @pl.when(n5 >= 0)
        def _():
            remote(g_buf.at[pl.ds(0, 7), n5], g_buf.at[pl.ds(0, 7), n5], a_ssem.at[0, 0], a_rsem.at[n5], partner).wait_recv()
            remote(hm_buf.at[pl.ds(0, 7), n5], hm_buf.at[pl.ds(0, 7), n5], h_ssem.at[0, 0], h_rsem.at[n5], partner).wait_recv()

            @pl.when(n5 < NT - 1)
            def _():
                for j in range(0, 8, 2):
                    finish(37 * (j // 2) + n5, g_buf[j, n5], hm_buf[j, n5, 0], hm_buf[j, n5, 1])

            @pl.when(n5 >= 1)
            def _():
                for j in range(1, 8, 2):
                    finish(37 * (j // 2) + 18 + n5, g_buf[j, n5], hm_buf[j, n5, 0], hm_buf[j, n5, 1])
        return carry

    lax.fori_loop(0, NT + 5, body, 0)

    for j in range(0, 8, 2):
        finish(37 * (j // 2) + 18, g_buf[j, NT - 1] + g_buf[j + 1, 0],
               hm_buf[j, NT - 1, 0] + hm_buf[j + 1, 0, 0], hm_buf[j, NT - 1, 1] + hm_buf[j + 1, 0, 1])
    first = pl.multiple_of(4 * 148 * h, 8)
    outs = [pltpu.make_async_copy(fresh.at[pl.ds(first, 4144), :], fresh_out, o_sem.at[0]),
            pltpu.make_async_copy(ratio.at[pl.ds(first, 4144), :], ratio_out, o_sem.at[1])]
    for c in outs:
        c.start()

    for n in range(NT - NS, NT):
        for c in x_copies(n):
            c.wait_send()
    for n in range(NT - NQ, NT):
        for c in z_copies(n):
            c.wait_send()
        for c in a_copies(n):
            c.wait_send()
        for c in h_copies(n):
            c.wait_send()
    for n in range(NT - 2, NT):
        d_copy(n).wait_send()
    for c in outs:
        c.wait()


def local(acts, cot, hess, mom, gamma_table, layer, steps):
    f32, bf16 = jnp.float32, jnp.bfloat16
    dma, vmem = pltpu.SemaphoreType.DMA, pltpu.VMEM
    anyspec = pl.BlockSpec(memory_space=pl.ANY)
    smem = pl.BlockSpec(memory_space=pltpu.SMEM)
    out = jax.ShapeDtypeStruct((4144, LANES), f32)
    fresh, ratio = pl.pallas_call(
        kernel,
        out_shape=(out, out),
        in_specs=[anyspec] * 4 + [smem] * 3,
        out_specs=(anyspec, anyspec),
        scratch_shapes=[
            vmem((2, 1792, 1024), bf16), vmem((2, 1024, 896), bf16), vmem((NT * LANES, 1024), bf16),
            vmem((224, 2368), f32), vmem((224, 2368), f32), vmem((2, 224, LANES), f32),
            vmem((2, 1792, LANES), f32), vmem((ND, 1792, LANES), f32), vmem((NS, 8, 224, LANES), f32),
            vmem((NT, 2, 224, LANES), f32), vmem((NT, 2, 224, LANES), f32), vmem((NT, 2, 224, LANES), f32),
            vmem((NQ, 2, 4, 56, LANES), f32), vmem((NT, 2, 4, WIN, LANES), f32), vmem((NQ, 2, 4, WIN, LANES), f32),
            vmem((8, NT, WIN, LANES), f32), vmem((NQ, 2, 4, 56, LANES), f32), vmem((8, NT, 2, WIN, LANES), f32),
            vmem((WIN * 148, LANES), f32), vmem((WIN * 148, LANES), f32),
            dma((4,)), dma((2,)), dma((2,)),
            dma((2,)), dma((ND,)), pltpu.SemaphoreType.REGULAR, dma((NS, 6)), dma((NT, 2)), dma((NT, 2)), dma((NT, 2)),
            dma((NQ, 2)), dma((NT, 2)), dma((NQ, 7)), dma((NT,)), dma((NQ, 7)), dma((NT,)), dma((2,)),
        ],
        compiler_params=pltpu.CompilerParams(collective_id=0, has_side_effects=True, vmem_limit_bytes=67043328),
    )(acts, cot.T, hess, mom, gamma_table, layer, steps)
    return fresh.reshape(-1), ratio.reshape(-1)


def solution(mesh):
    return jax.shard_map(
        local, mesh=mesh,
        in_specs=(P("dp", None), P("dp", "tensor"), P("dp", "tensor"), P("dp", "tensor"), P(None), P(None), P(None)),
        out_specs=(P(("dp", "tensor")), P(("dp", "tensor"))),
        check_vma=False)
```

```python
import jax
import jax.numpy as jnp
from jax import lax
from jax.experimental import pallas as pl
from jax.experimental.pallas import tpu as pltpu
from jax.sharding import PartitionSpec as P

TOKENS = 16384
MESH = pl.DeviceIdType.MESH
LANES = 128
WIN = 32

NT = 19
NZ = 3
NX = NT - NZ
HALF = NX - 1
NS = 4
ND = 3
NQ = 4
NH = 6


def kernel(acts, cot_t, hess, mom, gamma_table, layer, steps, fresh, ratio,
           acts_t, stage, cot, h_in, m_in, tail,
           d_send, d_recv, s_buf, far, direct, relay, q_buf, z_recv, a_send, g_buf, hm_send, hm_buf,
           zs, zf, far_z, direct_z, relay_z, az,
           ld_sem, cot_sem, st_sem,
           d0_ssem, d0_rsem, d_ssem, d_rsem, d_free, x_ssem, far_sem, direct_sem, relay_sem,
           z_ssem, z_rsem, a_ssem, a_rsem, h_ssem, h_rsem, zf_ssem, zf_rsem, xz_ssem, az_ssem):
    dp = lax.axis_index("dp")
    tn = lax.axis_index("tensor")
    core = lax.rem(dp, 2)
    m = lax.rem(lax.div(dp, 2), 2)
    x = lax.div(dp, 4)
    h = lax.rem(tn, 2)
    y = lax.div(tn, 2)

    def dp_of(x_, m_, core_):
        return (x_ * 2 + m_) * 2 + core_

    def x_at(k):
        return lax.rem(x + k, 4)

    partner = (dp_of(x, m, 1 - core), tn)
    right = (dp_of(x_at(1), m, core), tn)
    left = (dp_of(x_at(3), m, core), tn)
    flip_dp = dp_of(x, 1 - m, core)
    zpeer = (flip_dp, tn)

    barrier = pltpu.get_barrier_semaphore()
    peers = []
    for k in (2, 1, 3, 0):
        if k:
            peers.append((dp, lax.rem(y + k, 4) * 2 + h))
        peers.append((dp, lax.rem(y + k, 4) * 2 + 1 - h))
        peers.append((flip_dp, lax.rem(y + k, 4) * 2 + 1 - h))
    peers += [zpeer, left, right, partner]
    for peer in peers:
        pl.semaphore_signal(barrier, inc=1, device_id=peer, device_id_type=MESH)

    order = [x_at(2), x_at(1), x_at(3), x]
    cot_ld = [
        pltpu.make_async_copy(cot_t.at[pl.ds(lo, n)], cot.at[pl.ds(pl.multiple_of(lo + 64 * h, 64), n)], cot_sem.at[k])
        for k, (lo, n) in enumerate(((0, 192), (192, 2176)))
    ]
    acts_ld = [pltpu.make_async_copy(acts.at[:, pl.ds(pl.multiple_of(p * 896, LANES), 896)], stage.at[k % 2], ld_sem.at[k])
               for k, p in enumerate(order)]
    st_ld = [pltpu.make_async_copy(hess, h_in, st_sem.at[0]), pltpu.make_async_copy(mom, m_in, st_sem.at[1])]
    acts_ld[0].start()
    cot_ld[0].start()
    acts_ld[1].start()

    cot[pl.ds(pl.multiple_of((1 - h) * 2368, 64), 64), :] = jnp.zeros((64, 1024), jnp.bfloat16)

    def remote(src, dst, ssem, rsem, dev):
        return pltpu.make_async_remote_copy(src_ref=src, dst_ref=dst, send_sem=ssem, recv_sem=rsem,
                                            device_id=dev, device_id_type=MESH)

    def tile_of(n, h_):
        return jnp.where(n == HALF, (NT - 1) * (1 - h_), n + h_ - (n > HALF).astype(jnp.int32))

    def matmul(rows, n):
        return lax.dot_general(
            rows, cot[pl.ds(pl.multiple_of(tile_of(n, h) * LANES, LANES), LANES), :],
            (((1,), (1,)), ((), ())), preferred_element_type=jnp.float32)

    def product(which, n):
        return matmul(acts_t[which].reshape(1792, 1024), n).reshape(4, 448, LANES)

    def q_of_x(n):
        return n + jnp.minimum(lax.div(jnp.maximum(n - 2, 0), 4), NZ)

    def q_of_z(i):
        return 5 * i + 6

    def d0_copy(k):
        return remote(d_send.at[0, order[k]], d_recv.at[0, order[k]], d0_ssem.at[k], d0_rsem.at[k], partner)

    def d_copy(q):
        return remote(d_send.at[lax.rem(q, 2)], d_recv.at[lax.rem(q, ND)], d_ssem.at[lax.rem(q, 2)],
                      d_rsem.at[lax.rem(q, ND)], partner)

    def x_set(at, half_of, far_, direct_, relay_, ssem, fsem, dsem, rsem):
        return (
            remote(half_of(at(2), 0), far_.at[0], ssem.at[0], fsem.at[0], left),
            remote(half_of(at(2), 1), far_.at[1], ssem.at[1], fsem.at[1], right),
            remote(half_of(at(1), 0), direct_.at[0], ssem.at[2], dsem.at[0], right),
            remote(half_of(at(3), 1), direct_.at[1], ssem.at[3], dsem.at[1], left),
            remote(half_of(at(3), 0), relay_.at[0], ssem.at[4], rsem.at[0], left),
            remote(half_of(at(1), 1), relay_.at[1], ssem.at[5], rsem.at[1], right),
        )

    def blk(n, k, half):
        return s_buf.at[lax.rem(n, NS), x_at(k), half]

    def x_copies(n):
        return x_set(lambda k: s_buf.at[lax.rem(n, NS), x_at(k)], lambda r, half: r.at[half],
                     far.at[n], direct.at[n], relay.at[n], x_ssem.at[lax.rem(n, NS)],
                     far_sem.at[n], direct_sem.at[n], relay_sem.at[n])

    def half_copies():
        short = pl.ds(0, 112)
        return x_set(lambda k: s_buf.at[HALF % NS, x_at(k)], lambda r, half: r.at[half, short, :],
                     far.at[HALF, :, short, :], direct.at[HALF, :, short, :], relay.at[HALF, :, short, :],
                     x_ssem.at[HALF % NS], far_sem.at[HALF], direct_sem.at[HALF], relay_sem.at[HALF])

    def zblk(i, k, half):
        return zs.at[i, x_at(k), m, pl.ds(112 * half, 112), :]

    def xz_copies(i):
        return x_set(lambda k: zs.at[i, x_at(k), m], lambda r, half: r.at[pl.ds(112 * half, 112), :],
                     far_z.at[i], direct_z.at[i], relay_z.at[i], xz_ssem.at[i],
                     far_sem.at[NX + i], direct_sem.at[NX + i], relay_sem.at[NX + i])

    def zf_copy(i, k):
        return remote(zs.at[i, k, 1 - m], zf.at[i, k], zf_ssem.at[i, k], zf_rsem.at[i, k], zpeer)

    def z_copies(n):
        s = lax.rem(n, NQ)
        return (remote(q_buf.at[s, 1 - m, h], z_recv.at[n, 0], z_ssem.at[s, 0], z_rsem.at[n, 0], zpeer),
                remote(q_buf.at[s, m, 1 - h], z_recv.at[n, 1], z_ssem.at[s, 1], z_rsem.at[n, 1], zpeer))

    def window(to):
        return pl.ds(pl.multiple_of(28 * to - 4 * lax.rem(to, 2), 8), WIN)

    def a_copies(n):
        s = lax.rem(n, NQ)
        out = []
        for k in range(1, 4):
            to = lax.rem(y + k, 4)
            out.append(remote(a_send.at[s, 0, window(to), :], g_buf.at[tn, n], a_ssem.at[s, k - 1], a_rsem.at[n], (dp, to * 2 + h)))
        for k in range(4):
            to = lax.rem(y + k, 4)
            out.append(remote(a_send.at[s, 1, window(to), :], g_buf.at[tn, n], a_ssem.at[s, 3 + k], a_rsem.at[n], (flip_dp, to * 2 + 1 - h)))
        return out

    def az_copies(i):
        out = []
        for k in range(1, 8):
            to = lax.rem(tn + k, 8)
            out.append(remote(az.at[i, lax.rem(to, 2), window(lax.div(to, 2)), :], g_buf.at[tn, NX + i],
                              az_ssem.at[i, k - 1], a_rsem.at[NX + i], (dp, to)))
        return out

    def h_copies(n):
        s = lax.rem(n, NH)
        out = []
        for k in range(1, 8):
            to = lax.rem(tn + k, 8)
            out.append(remote(hm_send.at[s, :, lax.div(to, 2), pl.ds(pl.multiple_of(24 * lax.rem(to, 2), 8), WIN), :],
                              hm_buf.at[tn, n], h_ssem.at[s, k - 1], h_rsem.at[n], (dp, to)))
        return out

    def turn(k):
        for i in range(7):
            block = stage[k % 2, :, i * LANES:(i + 1) * LANES].T
            done = 0
            while done < LANES:
                which, inside = divmod(i * LANES + done, 224)
                size = min(224 - inside, LANES - done)
                dest = (which // 2) * 224 + inside
                acts_t[which % 2, order[k], dest:dest + size, :] = block[done:done + size]
                done += size

    def own_piece(k):
        p = order[k]
        own = matmul(acts_t[core, p], jnp.int32(0))
        d0_copy(k).wait_recv()
        s_buf[0, p] = (own + d_recv[0, p]).reshape(2, 224, LANES)

    first = x_copies(0)
    for k in range(4):
        acts_ld[k].wait()
        turn(k)
        if k < 2:
            acts_ld[k + 2].start()
        if k == 0:
            cot_ld[1].start()
            cot_ld[0].wait()
        if k == 1:
            st_ld[0].start()
            st_ld[1].start()
        d_send[0, order[k]] = matmul(acts_t[1 - core, order[k]], jnp.int32(0))
        if k == 0:
            pl.semaphore_wait(barrier, len(peers))
        d0_copy(k).start()
        if k == 1:
            own_piece(0)
            first[0].start()
            first[1].start()
        if k == 2:
            own_piece(1)
            first[2].start()
    own_piece(2)
    first[3].start()
    own_piece(3)
    pl.semaphore_signal(d_free, inc=1, device_id=partner, device_id_type=MESH)

    def pass_on(cs, at_half, far_):
        for half, at in ((0, 3), (1, 1)):
            cs[half].wait_recv()
            b = at_half(at, half)
            b[...] = b[...] + far_[half]
            cs[4 + half].start()

    def send_partial(n, q):
        @pl.when(q >= 3)
        def _():
            d_copy(q - 2).wait_send()
        d_send[lax.rem(q, 2)] = product(1 - core, n)

        @pl.when(q >= ND)
        def _():
            pl.semaphore_wait(d_free, 1)
        d_copy(q).start()

    cot_ld[1].wait()
    send_partial(jnp.int32(1), jnp.int32(1))
    pass_on(first, lambda k, half: blk(0, k, half), far.at[0])
    for k in range(4):
        d0_copy(k).wait_send()
    st_ld[0].wait()
    st_ld[1].wait()
    for k, ref in enumerate((h_in, m_in)):
        tail[k] = jnp.concatenate([ref[:, 2304:], jnp.zeros((224, 64), jnp.float32)], axis=1)

    correction_power = jnp.float32(1.0)
    count = steps[0]
    for bit in range(15):
        correction_power = jnp.where(lax.rem(lax.div(count, 2 ** bit), 2) == 1,
                                     correction_power * jnp.float32(0.99 ** (2 ** bit)), correction_power)
    correction = 1.0 - correction_power
    factor = correction / gamma_table[layer[0]]
    y_odd = lax.rem(y, 2) == 1

    def trim(v, odd):
        return jnp.where(odd, v[4:], v[:28])

    def finish(tile, g, hs, mo):
        g, hs, mo = trim(g, y_odd), trim(hs, h == 1), trim(mo, h == 1)
        new = 0.99 * hs + (0.01 / TOKENS) * (g * g)
        fresh[pl.ds(tile, 28, stride=148), :] = new
        ratio[pl.ds(tile, 28, stride=148), :] = jnp.clip(mo * factor / new, -1.0, 1.0)

    lane = lax.broadcasted_iota(jnp.int32, (224, LANES), 1)

    def state_tile(k, ref, n):
        at = lambda i: ref[:, pl.ds(pl.multiple_of(i * LANES, LANES), LANES)]
        here = jnp.where(n < NT - 1, at(jnp.minimum(n, NT - 2)), tail[k])
        before = jnp.where(n > 0, at(jnp.maximum(n - 1, 0)), 0.0)
        moved = jnp.where(lane < 64, pltpu.roll(before, 64, 1), pltpu.roll(here, 64, 1))
        return jnp.where(h == 0, here, moved)

    low = lane[:112] < 64

    def pack(v):
        a, b = v[:112], v[112:]
        return jnp.where(h == 0, a + pltpu.roll(b, 64, 1), pltpu.roll(a, 64, 1) + b)

    def unpack(v):
        w = pltpu.roll(v, 64, 1)
        a = jnp.where(h == 0, jnp.where(low, v, 0.0), jnp.where(low, 0.0, w))
        b = jnp.where(h == 0, jnp.where(low, w, 0.0), jnp.where(low, 0.0, v))
        return jnp.concatenate([a, b], axis=0)

    def states_before(t):
        n = jnp.where(t <= 3, 3 * t - 3, jnp.where(t <= 5, 2 * t, t + 5))
        return jnp.minimum(n, NT)

    def state_step(n, carry):
        s = lax.rem(n, NH)

        @pl.when(n >= NH)
        def _():
            for c in h_copies(n - NH):
                c.wait_send()
        hm_send[s, 0] = state_tile(0, h_in, tile_of(n, h)).reshape(4, 56, LANES)
        hm_send[s, 1] = state_tile(1, m_in, tile_of(n, h)).reshape(4, 56, LANES)
        hm_buf[tn, n] = hm_send[s, :, y, pl.ds(pl.multiple_of(24 * h, 8), WIN), :]
        for c in h_copies(n):
            c.start()
        return carry

    def by_z_hi(dst, v):
        for y_ in range(4):
            for z_ in range(2):
                dst[z_, 28 * y_:28 * y_ + 28, :] = v[56 * y_ + 28 * z_:56 * y_ + 28 * z_ + 28]

    def own_sum(n, q):
        own = product(core, n)
        d_copy(q).wait_recv()
        total = (own + d_recv[lax.rem(q, ND)]).reshape(4, 2, 224, LANES)

        return total

    def free(q):
        @pl.when(q < NT - ND)
        def _():
            pl.semaphore_signal(d_free, inc=1, device_id=partner, device_id_type=MESH)

    def within(n, lo, hi):
        return pl.when(jnp.logical_and(n >= lo, n < hi))

    def body(t, carry):
        @within(t, 1, NX)
        def _():
            q = q_of_x(t)

            @pl.when(t >= NS)
            def _():
                for c in x_copies(t - NS):
                    c.wait_send()

            @pl.when(t < HALF)
            def _():
                s_buf[lax.rem(t, NS)] = own_sum(t, q)
                for c in x_copies(t)[:4]:
                    c.start()

            @pl.when(t == HALF)
            def _():
                total = own_sum(t, q)
                for k in range(4):
                    for half in range(2):
                        s_buf[HALF % NS, k, half, pl.ds(0, 112), :] = pack(total[k, half])
                for c in half_copies()[:4]:
                    c.start()
            free(q)

        @pl.when(t + 1 < NX)
        def _():
            send_partial(t + 1, q_of_x(t + 1))

        zi = lax.div(t - 5, 4)

        @pl.when(jnp.logical_and(lax.rem(t, 4) == 1, jnp.logical_and(t >= 5, t <= 4 * NZ + 1)))
        def _():
            q = q_of_z(zi)
            zs[zi] = own_sum(NX + zi, q)
            free(q)

        @within(t, 5, 5 + 4 * NZ)
        def _():
            zf_copy(zi, lax.rem(t - 5 + x + 2, 4)).start()

        @within(t, NX, NT)
        def _():
            i = t - NX
            cs = xz_copies(i)
            for k, go in ((2, (0, 1)), (1, (2,)), (3, (3,)), (0, ())):
                zf_copy(i, x_at(k)).wait_recv()
                zs[i, x_at(k), m] = zs[i, x_at(k), m] + zf[i, x_at(k)]
                for g in go:
                    cs[g].start()

        u2 = t - 1

        @within(u2, 1, HALF)
        def _():
            pass_on(x_copies(u2), lambda k, half: blk(u2, k, half), far.at[u2])

        @pl.when(u2 == HALF)
        def _():
            short = pl.ds(0, 112)
            pass_on(half_copies(), lambda k, half: s_buf.at[HALF % NS, x_at(k), half, short, :], far.at[HALF, :, short, :])

        @within(u2, NX, NT)
        def _():
            i = u2 - NX
            pass_on(xz_copies(i), lambda k, half: zblk(i, k, half), far_z.at[i])

        @pl.when(jnp.logical_and(lax.rem(t, 4) == 0, jnp.logical_and(t >= 4, t <= 4 * NZ)))
        def _():
            send_partial(NX + lax.div(t - 4, 4), q_of_z(lax.div(t - 4, 4)))

        lax.fori_loop(states_before(t), states_before(t + 1), state_step, 0)

        u3 = t - 3

        @within(u3, 0, NX)
        def _():
            @pl.when(u3 >= NQ)
            def _():
                for c in z_copies(u3 - NQ):
                    c.wait_send()
            s = lax.rem(u3, NQ)

            @pl.when(u3 < HALF)
            def _():
                cs = x_copies(u3)
                for half in range(2):
                    cs[2 + half].wait_recv()
                    cs[4 + half].wait_recv()
                    by_z_hi(q_buf.at[s, half], blk(u3, 0, half)[...] + direct[u3, half] + relay[u3, half])

            @pl.when(u3 == HALF)
            def _():
                cs = half_copies()
                for half in range(2):
                    cs[2 + half].wait_recv()
                    cs[4 + half].wait_recv()
                    total = s_buf[HALF % NS, x, half, :112] + direct[HALF, half, :112] + relay[HALF, half, :112]
                    by_z_hi(q_buf.at[s, half], unpack(total))
            for c in z_copies(u3):
                c.start()

        @within(u3, NX, NT)
        def _():
            i = u3 - NX
            cs = xz_copies(i)
            halves = []
            for half in range(2):
                cs[2 + half].wait_recv()
                cs[4 + half].wait_recv()
                halves.append(zblk(i, 0, half)[...] + direct_z[i, half] + relay_z[i, half])
            by_z_hi(az.at[i], jnp.concatenate(halves, axis=0))
            g_buf[tn, NX + i] = az[i, h, window(y), :]
            for c in az_copies(i):
                c.start()

        u4 = t - 5

        @within(u4, 0, NX)
        def _():
            s = lax.rem(u4, NQ)

            @pl.when(u4 >= NQ)
            def _():
                for c in a_copies(u4 - NQ):
                    c.wait_send()
            for c in z_copies(u4):
                c.wait_recv()
            a_send[s, 0] = q_buf[s, m, h] + z_recv[u4, 0]
            a_send[s, 1] = q_buf[s, 1 - m, 1 - h] + z_recv[u4, 1]
            g_buf[tn, u4] = a_send[s, 0, window(y), :]
            for c in a_copies(u4):
                c.start()

        u5 = t - 7

        @pl.when(u5 >= 0)
        def _():
            remote(g_buf.at[pl.ds(0, 7), u5], g_buf.at[pl.ds(0, 7), u5], a_ssem.at[0, 0], a_rsem.at[u5], partner).wait_recv()
            remote(hm_buf.at[pl.ds(0, 7), u5], hm_buf.at[pl.ds(0, 7), u5], h_ssem.at[0, 0], h_rsem.at[u5], partner).wait_recv()

            @pl.when(u5 != HALF)
            def _():
                for j in range(8):
                    finish(37 * (j // 2) + 18 * (j % 2) + tile_of(u5, j % 2), g_buf[j, u5], hm_buf[j, u5, 0], hm_buf[j, u5, 1])

            @pl.when(u5 == HALF)
            def _():
                for j in range(0, 8, 2):
                    finish(37 * (j // 2) + 18, *(a + b for a, b in (
                        (g_buf[j, HALF], g_buf[j + 1, HALF]),
                        (hm_buf[j, HALF, 0], hm_buf[j + 1, HALF, 0]), (hm_buf[j, HALF, 1], hm_buf[j + 1, HALF, 1]))))
        return carry

    lax.fori_loop(1, NT + 7, body, 0)

    for n in range(NX - NS, NX):
        for c in half_copies() if n == HALF else x_copies(n):
            c.wait_send()
    for n in range(NX - NQ, NX):
        for c in z_copies(n) + tuple(a_copies(n)):
            c.wait_send()
    for n in range(NT - NH, NT):
        for c in h_copies(n):
            c.wait_send()
    for i in range(NZ):
        for k in range(4):
            zf_copy(i, k).wait_send()
        for c in xz_copies(i) + tuple(az_copies(i)):
            c.wait_send()
    for q in range(NT - 2, NT):
        d_copy(q).wait_send()


def local(acts, cot, hess, mom, gamma_table, layer, steps):
    f32, bf16 = jnp.float32, jnp.bfloat16
    dma, vmem = pltpu.SemaphoreType.DMA, pltpu.VMEM
    anyspec = pl.BlockSpec(memory_space=pl.ANY)
    smem = pl.BlockSpec(memory_space=pltpu.SMEM)
    out = pltpu.VMEM((4144, LANES), f32)
    fresh, ratio = pl.pallas_call(
        kernel,
        out_shape=(out, out),
        in_specs=[anyspec] * 4 + [smem] * 3,
        out_specs=(pl.BlockSpec(memory_space=pltpu.VMEM),) * 2,
        scratch_shapes=[
            vmem((2, 4, 448, 1024), bf16), vmem((2, 1024, 896), bf16), vmem((NT * LANES, 1024), bf16),
            vmem((224, 2368), f32), vmem((224, 2368), f32), vmem((2, 224, LANES), f32),
            vmem((2, 4, 448, LANES), f32), vmem((ND, 4, 448, LANES), f32), vmem((NS, 4, 2, 224, LANES), f32),
            vmem((NX, 2, 224, LANES), f32), vmem((NX, 2, 224, LANES), f32), vmem((NX, 2, 224, LANES), f32),
            vmem((NQ, 2, 2, 112, LANES), f32), vmem((NX, 2, 112, LANES), f32), vmem((NQ, 2, 112, LANES), f32),
            vmem((8, NT, WIN, LANES), f32), vmem((NH, 2, 4, 56, LANES), f32), vmem((8, NT, 2, WIN, LANES), f32),
            vmem((NZ, 4, 2, 224, LANES), f32), vmem((NZ, 4, 224, LANES), f32),
            vmem((NZ, 2, 112, LANES), f32), vmem((NZ, 2, 112, LANES), f32), vmem((NZ, 2, 112, LANES), f32),
            vmem((NZ, 2, 112, LANES), f32),
            dma((4,)), dma((2,)), dma((2,)),
            dma((4,)), dma((4,)), dma((2,)), dma((ND,)), pltpu.SemaphoreType.REGULAR,
            dma((NS, 6)), dma((NT, 2)), dma((NT, 2)), dma((NT, 2)),
            dma((NQ, 2)), dma((NX, 2)), dma((NQ, 7)), dma((NT,)), dma((NH, 7)), dma((NT,)),
            dma((NZ, 4)), dma((NZ, 4)), dma((NZ, 6)), dma((NZ, 7)),
        ],
        compiler_params=pltpu.CompilerParams(collective_id=0, has_side_effects=True, vmem_limit_bytes=62500000),
    )(acts, cot.T, hess, mom, gamma_table, layer, steps)
    return fresh.reshape(-1), ratio.reshape(-1)


def solution(mesh):
    return jax.shard_map(
        local, mesh=mesh,
        in_specs=(P("dp", None), P("dp", "tensor"), P("dp", "tensor"), P("dp", "tensor"), P(None), P(None), P(None)),
        out_specs=(P(("dp", "tensor")), P(("dp", "tensor"))),
        check_vma=False)
```

```python
import jax
import jax.numpy as jnp
from jax import lax
from jax.experimental import pallas as pl
from jax.experimental.pallas import tpu as pltpu
from jax.sharding import PartitionSpec as P

TOKENS = 16384
MESH = pl.DeviceIdType.MESH
LANES = 128
WIN = 32

NT = 19
NZ = 3
NX = NT - NZ
HALF = NX - 1
NS = 4
ND = 3
NQ = 6
NH = 6


def kernel(acts, cot_t, hess, mom, gamma_table, layer, steps, fresh, ratio,
           acts_t, stage, cot, h_in, m_in, tail,
           d_send, d_recv, s_buf, far, direct, relay, q_buf, z_recv, a_send, g_buf, hm_send, hm_buf,
           zs, zf, far_z, direct_z, relay_z, az,
           ld_sem, cot_sem, st_sem,
           d0_ssem, d0_rsem, d_ssem, d_rsem, d_free, x_ssem, far_sem, direct_sem, relay_sem,
           z_ssem, z_rsem, a_ssem, a_rsem, h_ssem, h_rsem, zf_ssem, zf_rsem, xz_ssem, az_ssem):
    dp = lax.axis_index("dp")
    tn = lax.axis_index("tensor")
    core = lax.rem(dp, 2)
    m = lax.rem(lax.div(dp, 2), 2)
    x = lax.div(dp, 4)
    h = lax.rem(tn, 2)
    y = lax.div(tn, 2)

    def dp_of(x_, m_, core_):
        return (x_ * 2 + m_) * 2 + core_

    def x_at(k):
        return lax.rem(x + k, 4)

    partner = (dp_of(x, m, 1 - core), tn)
    right = (dp_of(x_at(1), m, core), tn)
    left = (dp_of(x_at(3), m, core), tn)
    flip_dp = dp_of(x, 1 - m, core)
    zpeer = (flip_dp, tn)

    barrier = pltpu.get_barrier_semaphore()
    peers = []
    for k in (2, 1, 3, 0):
        if k:
            peers.append((dp, lax.rem(y + k, 4) * 2 + h))
        peers.append((dp, lax.rem(y + k, 4) * 2 + 1 - h))
        peers.append((flip_dp, lax.rem(y + k, 4) * 2 + 1 - h))
    peers += [zpeer, left, right, partner]
    for peer in peers:
        pl.semaphore_signal(barrier, inc=1, device_id=peer, device_id_type=MESH)

    order = [x_at(2), x_at(1), x_at(3), x]
    cot_ld = [
        pltpu.make_async_copy(cot_t.at[pl.ds(lo, n)], cot.at[pl.ds(pl.multiple_of(lo + 64 * h, 64), n)], cot_sem.at[k])
        for k, (lo, n) in enumerate(((0, 192), (192, 2176)))
    ]
    acts_ld = [pltpu.make_async_copy(acts.at[:, pl.ds(pl.multiple_of(p * 896, LANES), 896)], stage.at[k % 2], ld_sem.at[k])
               for k, p in enumerate(order)]
    st_ld = [pltpu.make_async_copy(hess, h_in, st_sem.at[0]), pltpu.make_async_copy(mom, m_in, st_sem.at[1])]
    acts_ld[0].start()
    cot_ld[0].start()
    acts_ld[1].start()

    cot[pl.ds(pl.multiple_of((1 - h) * 2368, 64), 64), :] = jnp.zeros((64, 1024), jnp.bfloat16)

    def remote(src, dst, ssem, rsem, dev):
        return pltpu.make_async_remote_copy(src_ref=src, dst_ref=dst, send_sem=ssem, recv_sem=rsem,
                                            device_id=dev, device_id_type=MESH)

    def tile_of(n, h_):
        return jnp.where(n == HALF, (NT - 1) * (1 - h_), n + h_ - (n > HALF).astype(jnp.int32))

    def matmul(rows, n):
        return lax.dot_general(
            rows, cot[pl.ds(pl.multiple_of(tile_of(n, h) * LANES, LANES), LANES), :],
            (((1,), (1,)), ((), ())), preferred_element_type=jnp.float32)

    def product(which, n):
        return matmul(acts_t[which].reshape(1792, 1024), n).reshape(4, 448, LANES)

    def q_of_x(n):
        return n + jnp.minimum(lax.div(jnp.maximum(n - 2, 0), 4), NZ)

    def q_of_z(i):
        return 5 * i + 6

    def d0_copy(k):
        return remote(d_send.at[0, order[k]], d_recv.at[0, order[k]], d0_ssem.at[k], d0_rsem.at[k], partner)

    def d_copy(q):
        return remote(d_send.at[lax.rem(q, 2)], d_recv.at[lax.rem(q, ND)], d_ssem.at[lax.rem(q, 2)],
                      d_rsem.at[lax.rem(q, ND)], partner)

    def x_set(at, half_of, far_, direct_, relay_, ssem, fsem, dsem, rsem):
        return (
            remote(half_of(at(2), 0), far_.at[0], ssem.at[0], fsem.at[0], left),
            remote(half_of(at(2), 1), far_.at[1], ssem.at[1], fsem.at[1], right),
            remote(half_of(at(1), 0), direct_.at[0], ssem.at[2], dsem.at[0], right),
            remote(half_of(at(3), 1), direct_.at[1], ssem.at[3], dsem.at[1], left),
            remote(half_of(at(3), 0), relay_.at[0], ssem.at[4], rsem.at[0], left),
            remote(half_of(at(1), 1), relay_.at[1], ssem.at[5], rsem.at[1], right),
        )

    def blk(n, k, half):
        return s_buf.at[lax.rem(n, NS), x_at(k), half]

    def x_copies(n):
        return x_set(lambda k: s_buf.at[lax.rem(n, NS), x_at(k)], lambda r, half: r.at[half],
                     far.at[n], direct.at[n], relay.at[n], x_ssem.at[lax.rem(n, NS)],
                     far_sem.at[n], direct_sem.at[n], relay_sem.at[n])

    def half_copies():
        short = pl.ds(0, 112)
        return x_set(lambda k: s_buf.at[HALF % NS, x_at(k)], lambda r, half: r.at[half, short, :],
                     far.at[HALF, :, short, :], direct.at[HALF, :, short, :], relay.at[HALF, :, short, :],
                     x_ssem.at[HALF % NS], far_sem.at[HALF], direct_sem.at[HALF], relay_sem.at[HALF])

    def zblk(i, k, half):
        return zs.at[i, x_at(k), m, pl.ds(112 * half, 112), :]

    def xz_copies(i):
        return x_set(lambda k: zs.at[i, x_at(k), m], lambda r, half: r.at[pl.ds(112 * half, 112), :],
                     far_z.at[i], direct_z.at[i], relay_z.at[i], xz_ssem.at[i],
                     far_sem.at[NX + i], direct_sem.at[NX + i], relay_sem.at[NX + i])

    def zf_copy(i, k):
        return remote(zs.at[i, k, 1 - m], zf.at[i, k], zf_ssem.at[i, k], zf_rsem.at[i, k], zpeer)

    def z_copies(n):
        s = lax.rem(n, NQ)
        return (remote(q_buf.at[s, 1 - m, h], z_recv.at[n, 0], z_ssem.at[s, 0], z_rsem.at[n, 0], zpeer),
                remote(q_buf.at[s, m, 1 - h], z_recv.at[n, 1], z_ssem.at[s, 1], z_rsem.at[n, 1], zpeer))

    def window(to):
        return pl.ds(pl.multiple_of(28 * to - 4 * lax.rem(to, 2), 8), WIN)

    def a_copies(n):
        s = lax.rem(n, NQ)
        out = []
        for k in range(1, 4):
            to = lax.rem(y + k, 4)
            out.append(remote(a_send.at[s, 0, window(to), :], g_buf.at[tn, n], a_ssem.at[s, k - 1], a_rsem.at[n], (dp, to * 2 + h)))
        for k in range(4):
            to = lax.rem(y + k, 4)
            out.append(remote(a_send.at[s, 1, window(to), :], g_buf.at[tn, n], a_ssem.at[s, 3 + k], a_rsem.at[n], (flip_dp, to * 2 + 1 - h)))
        return out

    def az_copies(i):
        out = []
        for k in range(1, 8):
            to = lax.rem(tn + k, 8)
            out.append(remote(az.at[i, lax.rem(to, 2), window(lax.div(to, 2)), :], g_buf.at[tn, NX + i],
                              az_ssem.at[i, k - 1], a_rsem.at[NX + i], (dp, to)))
        return out

    def h_copies(n):
        s = lax.rem(n, NH)
        out = []
        for k in range(1, 8):
            to = lax.rem(tn + k, 8)
            out.append(remote(hm_send.at[s, :, lax.div(to, 2), pl.ds(pl.multiple_of(24 * lax.rem(to, 2), 8), WIN), :],
                              hm_buf.at[tn, n], h_ssem.at[s, k - 1], h_rsem.at[n], (dp, to)))
        return out

    def turn(k):
        for i in range(7):
            block = stage[k % 2, :, i * LANES:(i + 1) * LANES].T
            done = 0
            while done < LANES:
                which, inside = divmod(i * LANES + done, 224)
                size = min(224 - inside, LANES - done)
                dest = (which // 2) * 224 + inside
                acts_t[which % 2, order[k], dest:dest + size, :] = block[done:done + size]
                done += size

    def own_piece(k):
        p = order[k]
        own = matmul(acts_t[core, p], jnp.int32(0))
        d0_copy(k).wait_recv()
        s_buf[0, p] = (own + d_recv[0, p]).reshape(2, 224, LANES)

    first = x_copies(0)
    for k in range(4):
        acts_ld[k].wait()
        turn(k)
        if k < 2:
            acts_ld[k + 2].start()
        if k == 0:
            cot_ld[1].start()
            cot_ld[0].wait()
        if k == 1:
            st_ld[0].start()
            st_ld[1].start()
        d_send[0, order[k]] = matmul(acts_t[1 - core, order[k]], jnp.int32(0))
        if k == 0:
            pl.semaphore_wait(barrier, len(peers))
        d0_copy(k).start()
        if k == 1:
            own_piece(0)
            first[0].start()
            first[1].start()
        if k == 2:
            own_piece(1)
            first[2].start()
    own_piece(2)
    first[3].start()
    own_piece(3)
    pl.semaphore_signal(d_free, inc=1, device_id=partner, device_id_type=MESH)

    def pass_on(cs, at_half, far_):
        for half, at in ((0, 3), (1, 1)):
            cs[half].wait_recv()
            b = at_half(at, half)
            b[...] = b[...] + far_[half]
            cs[4 + half].start()

    def send_partial(n, q):
        @pl.when(q >= 3)
        def _():
            d_copy(q - 2).wait_send()
        d_send[lax.rem(q, 2)] = product(1 - core, n)

        @pl.when(q >= ND)
        def _():
            pl.semaphore_wait(d_free, 1)
        d_copy(q).start()

    cot_ld[1].wait()
    send_partial(jnp.int32(1), jnp.int32(1))
    pass_on(first, lambda k, half: blk(0, k, half), far.at[0])
    for k in range(4):
        d0_copy(k).wait_send()
    st_ld[0].wait()
    st_ld[1].wait()
    for k, ref in enumerate((h_in, m_in)):
        tail[k] = jnp.concatenate([ref[:, 2304:], jnp.zeros((224, 64), jnp.float32)], axis=1)

    correction_power = jnp.float32(1.0)
    count = steps[0]
    for bit in range(15):
        correction_power = jnp.where(lax.rem(lax.div(count, 2 ** bit), 2) == 1,
                                     correction_power * jnp.float32(0.99 ** (2 ** bit)), correction_power)
    correction = 1.0 - correction_power
    factor = correction / gamma_table[layer[0]]
    y_odd = lax.rem(y, 2) == 1

    def trim(v, odd):
        return jnp.where(odd, v[4:], v[:28])

    def finish(tile, g, hs, mo):
        g, hs, mo = trim(g, y_odd), trim(hs, h == 1), trim(mo, h == 1)
        new = 0.99 * hs + (0.01 / TOKENS) * (g * g)
        fresh[pl.ds(tile, 28, stride=148), :] = new
        ratio[pl.ds(tile, 28, stride=148), :] = jnp.clip(mo * factor / new, -1.0, 1.0)

    lane = lax.broadcasted_iota(jnp.int32, (224, LANES), 1)

    def state_tile(k, ref, n):
        at = lambda i: ref[:, pl.ds(pl.multiple_of(i * LANES, LANES), LANES)]
        here = jnp.where(n < NT - 1, at(jnp.minimum(n, NT - 2)), tail[k])
        before = jnp.where(n > 0, at(jnp.maximum(n - 1, 0)), 0.0)
        moved = jnp.where(lane < 64, pltpu.roll(before, 64, 1), pltpu.roll(here, 64, 1))
        return jnp.where(h == 0, here, moved)

    low = lane[:112] < 64

    def pack(v):
        a, b = v[:112], v[112:]
        return jnp.where(h == 0, a + pltpu.roll(b, 64, 1), pltpu.roll(a, 64, 1) + b)

    def unpack(v):
        w = pltpu.roll(v, 64, 1)
        a = jnp.where(h == 0, jnp.where(low, v, 0.0), jnp.where(low, 0.0, w))
        b = jnp.where(h == 0, jnp.where(low, w, 0.0), jnp.where(low, 0.0, v))
        return jnp.concatenate([a, b], axis=0)

    def states_before(t):
        n = jnp.where(t <= 3, 3 * t - 3, jnp.where(t <= 5, 2 * t, t + 5))
        return jnp.minimum(n, NT)

    def state_step(n, carry):
        s = lax.rem(n, NH)

        @pl.when(n >= NH)
        def _():
            for c in h_copies(n - NH):
                c.wait_send()
        hm_send[s, 0] = state_tile(0, h_in, tile_of(n, h)).reshape(4, 56, LANES)
        hm_send[s, 1] = state_tile(1, m_in, tile_of(n, h)).reshape(4, 56, LANES)
        hm_buf[tn, n] = hm_send[s, :, y, pl.ds(pl.multiple_of(24 * h, 8), WIN), :]
        for c in h_copies(n):
            c.start()
        return carry

    def by_z_hi(dst, v):
        for y_ in range(4):
            for z_ in range(2):
                dst[z_, 28 * y_:28 * y_ + 28, :] = v[56 * y_ + 28 * z_:56 * y_ + 28 * z_ + 28]

    def own_sum(n, q):
        own = product(core, n)
        d_copy(q).wait_recv()
        total = (own + d_recv[lax.rem(q, ND)]).reshape(4, 2, 224, LANES)

        return total

    def free(q):
        @pl.when(q < NT - ND)
        def _():
            pl.semaphore_signal(d_free, inc=1, device_id=partner, device_id_type=MESH)

    def within(n, lo, hi):
        return pl.when(jnp.logical_and(n >= lo, n < hi))

    def body(t, carry):
        @within(t, 1, NX)
        def _():
            q = q_of_x(t)

            @pl.when(t >= NS)
            def _():
                for c in x_copies(t - NS):
                    c.wait_send()

            @pl.when(t < HALF)
            def _():
                s_buf[lax.rem(t, NS)] = own_sum(t, q)
                for c in x_copies(t)[:4]:
                    c.start()

            @pl.when(t == HALF)
            def _():
                total = own_sum(t, q)
                for k in range(4):
                    for half in range(2):
                        s_buf[HALF % NS, k, half, pl.ds(0, 112), :] = pack(total[k, half])
                for c in half_copies()[:4]:
                    c.start()
            free(q)

        @pl.when(t + 1 < NX)
        def _():
            send_partial(t + 1, q_of_x(t + 1))

        zi = lax.div(t - 5, 4)

        @pl.when(jnp.logical_and(lax.rem(t, 4) == 1, jnp.logical_and(t >= 5, t <= 4 * NZ + 1)))
        def _():
            q = q_of_z(zi)
            zs[zi] = own_sum(NX + zi, q)
            free(q)

        @within(t, 5, 5 + 4 * NZ)
        def _():
            zf_copy(zi, lax.rem(t - 5 + x + 2, 4)).start()

        @within(t, NX, NT)
        def _():
            i = t - NX
            cs = xz_copies(i)
            for k, go in ((2, (0, 1)), (1, (2,)), (3, (3,)), (0, ())):
                zf_copy(i, x_at(k)).wait_recv()
                zs[i, x_at(k), m] = zs[i, x_at(k), m] + zf[i, x_at(k)]
                for g in go:
                    cs[g].start()

        u2 = t - 1

        @within(u2, 1, HALF)
        def _():
            pass_on(x_copies(u2), lambda k, half: blk(u2, k, half), far.at[u2])

        @pl.when(u2 == HALF)
        def _():
            short = pl.ds(0, 112)
            pass_on(half_copies(), lambda k, half: s_buf.at[HALF % NS, x_at(k), half, short, :], far.at[HALF, :, short, :])

        @within(u2, NX, NT)
        def _():
            i = u2 - NX
            pass_on(xz_copies(i), lambda k, half: zblk(i, k, half), far_z.at[i])

        @pl.when(jnp.logical_and(lax.rem(t, 4) == 0, jnp.logical_and(t >= 4, t <= 4 * NZ)))
        def _():
            send_partial(NX + lax.div(t - 4, 4), q_of_z(lax.div(t - 4, 4)))

        lax.fori_loop(states_before(t), states_before(t + 1), state_step, 0)

        u3 = t - 3

        @within(u3, 0, NX)
        def _():
            @pl.when(u3 >= NQ)
            def _():
                for c in z_copies(u3 - NQ):
                    c.wait_send()
            s = lax.rem(u3, NQ)

            @pl.when(u3 < HALF)
            def _():
                cs = x_copies(u3)
                for half in range(2):
                    cs[2 + half].wait_recv()
                    cs[4 + half].wait_recv()
                    by_z_hi(q_buf.at[s, half], blk(u3, 0, half)[...] + direct[u3, half] + relay[u3, half])

            @pl.when(u3 == HALF)
            def _():
                cs = half_copies()
                for half in range(2):
                    cs[2 + half].wait_recv()
                    cs[4 + half].wait_recv()
                    total = s_buf[HALF % NS, x, half, :112] + direct[HALF, half, :112] + relay[HALF, half, :112]
                    by_z_hi(q_buf.at[s, half], unpack(total))
            for c in z_copies(u3):
                c.start()

        @within(u3, NX, NT)
        def _():
            i = u3 - NX
            cs = xz_copies(i)
            halves = []
            for half in range(2):
                cs[2 + half].wait_recv()
                cs[4 + half].wait_recv()
                halves.append(zblk(i, 0, half)[...] + direct_z[i, half] + relay_z[i, half])
            by_z_hi(az.at[i], jnp.concatenate(halves, axis=0))
            g_buf[tn, NX + i] = az[i, h, window(y), :]
            for c in az_copies(i):
                c.start()

        u4 = t - 6

        @within(u4, 0, NX)
        def _():
            s = lax.rem(u4, NQ)

            @pl.when(u4 >= NQ)
            def _():
                for c in a_copies(u4 - NQ):
                    c.wait_send()
            for c in z_copies(u4):
                c.wait_recv()
            a_send[s, 0] = q_buf[s, m, h] + z_recv[u4, 0]
            a_send[s, 1] = q_buf[s, 1 - m, 1 - h] + z_recv[u4, 1]
            g_buf[tn, u4] = a_send[s, 0, window(y), :]
            for c in a_copies(u4):
                c.start()

        u5 = t - 9

        @pl.when(u5 >= 0)
        def _():
            remote(g_buf.at[pl.ds(0, 7), u5], g_buf.at[pl.ds(0, 7), u5], a_ssem.at[0, 0], a_rsem.at[u5], partner).wait_recv()
            remote(hm_buf.at[pl.ds(0, 7), u5], hm_buf.at[pl.ds(0, 7), u5], h_ssem.at[0, 0], h_rsem.at[u5], partner).wait_recv()

            @pl.when(u5 != HALF)
            def _():
                for j in range(8):
                    finish(37 * (j // 2) + 18 * (j % 2) + tile_of(u5, j % 2), g_buf[j, u5], hm_buf[j, u5, 0], hm_buf[j, u5, 1])

            @pl.when(u5 == HALF)
            def _():
                for j in range(0, 8, 2):
                    finish(37 * (j // 2) + 18, *(a + b for a, b in (
                        (g_buf[j, HALF], g_buf[j + 1, HALF]),
                        (hm_buf[j, HALF, 0], hm_buf[j + 1, HALF, 0]), (hm_buf[j, HALF, 1], hm_buf[j + 1, HALF, 1]))))
        return carry

    lax.fori_loop(1, NT + 9, body, 0)

    for n in range(NX - NS, NX):
        for c in half_copies() if n == HALF else x_copies(n):
            c.wait_send()
    for n in range(NX - NQ, NX):
        for c in z_copies(n) + tuple(a_copies(n)):
            c.wait_send()
    for n in range(NT - NH, NT):
        for c in h_copies(n):
            c.wait_send()
    for i in range(NZ):
        for k in range(4):
            zf_copy(i, k).wait_send()
        for c in xz_copies(i) + tuple(az_copies(i)):
            c.wait_send()
    for q in range(NT - 2, NT):
        d_copy(q).wait_send()


def local(acts, cot, hess, mom, gamma_table, layer, steps):
    f32, bf16 = jnp.float32, jnp.bfloat16
    dma, vmem = pltpu.SemaphoreType.DMA, pltpu.VMEM
    anyspec = pl.BlockSpec(memory_space=pl.ANY)
    smem = pl.BlockSpec(memory_space=pltpu.SMEM)
    out = pltpu.VMEM((4144, LANES), f32)
    fresh, ratio = pl.pallas_call(
        kernel,
        out_shape=(out, out),
        in_specs=[anyspec] * 4 + [smem] * 3,
        out_specs=(pl.BlockSpec(memory_space=pltpu.VMEM),) * 2,
        scratch_shapes=[
            vmem((2, 4, 448, 1024), bf16), vmem((2, 1024, 896), bf16), vmem((NT * LANES, 1024), bf16),
            vmem((224, 2368), f32), vmem((224, 2368), f32), vmem((2, 224, LANES), f32),
            vmem((2, 4, 448, LANES), f32), vmem((ND, 4, 448, LANES), f32), vmem((NS, 4, 2, 224, LANES), f32),
            vmem((NX, 2, 224, LANES), f32), vmem((NX, 2, 224, LANES), f32), vmem((NX, 2, 224, LANES), f32),
            vmem((NQ, 2, 2, 112, LANES), f32), vmem((NX, 2, 112, LANES), f32), vmem((NQ, 2, 112, LANES), f32),
            vmem((8, NT, WIN, LANES), f32), vmem((NH, 2, 4, 56, LANES), f32), vmem((8, NT, 2, WIN, LANES), f32),
            vmem((NZ, 4, 2, 224, LANES), f32), vmem((NZ, 4, 224, LANES), f32),
            vmem((NZ, 2, 112, LANES), f32), vmem((NZ, 2, 112, LANES), f32), vmem((NZ, 2, 112, LANES), f32),
            vmem((NZ, 2, 112, LANES), f32),
            dma((4,)), dma((2,)), dma((2,)),
            dma((4,)), dma((4,)), dma((2,)), dma((ND,)), pltpu.SemaphoreType.REGULAR,
            dma((NS, 6)), dma((NT, 2)), dma((NT, 2)), dma((NT, 2)),
            dma((NQ, 2)), dma((NX, 2)), dma((NQ, 7)), dma((NT,)), dma((NH, 7)), dma((NT,)),
            dma((NZ, 4)), dma((NZ, 4)), dma((NZ, 6)), dma((NZ, 7)),
        ],
        compiler_params=pltpu.CompilerParams(collective_id=0, has_side_effects=True, vmem_limit_bytes=62500000),
    )(acts, cot.T, hess, mom, gamma_table, layer, steps)
    return fresh.reshape(-1), ratio.reshape(-1)


def solution(mesh):
    return jax.shard_map(
        local, mesh=mesh,
        in_specs=(P("dp", None), P("dp", "tensor"), P("dp", "tensor"), P("dp", "tensor"), P(None), P(None), P(None)),
        out_specs=(P(("dp", "tensor")), P(("dp", "tensor"))),
        check_vma=False)
```

```python
import jax
import jax.numpy as jnp
from jax import lax
from jax.experimental import pallas as pl
from jax.experimental.pallas import tpu as pltpu
from jax.sharding import PartitionSpec as P

TOKENS = 16384
MESH = pl.DeviceIdType.MESH
LANES = 128
WIN = 32

NT = 19
NZ = 3
NX = NT - NZ
HALF = NX - 1
NS = 4
ND = 3
NQ = 6
NH = 6


def kernel(acts, cot_t, hess, mom, gamma_table, layer, steps, fresh, ratio,
           acts_t, stage, cot, h_in, m_in, tail,
           d_send, d_recv, s_buf, far, direct, relay, q_buf, z_recv, a_send, g_buf, hm_send, hm_buf,
           zs, zf, far_z, direct_z, relay_z, az,
           ld_sem, cot_sem, st_sem,
           d0_ssem, d0_rsem, d_ssem, d_rsem, d_free, x_ssem, far_sem, direct_sem, relay_sem,
           z_ssem, z_rsem, a_ssem, a_rsem, h_ssem, h_rsem, zf_ssem, zf_rsem, xz_ssem, az_ssem):
    dp = lax.axis_index("dp")
    tn = lax.axis_index("tensor")
    core = lax.rem(dp, 2)
    m = lax.rem(lax.div(dp, 2), 2)
    x = lax.div(dp, 4)
    h = lax.rem(tn, 2)
    y = lax.div(tn, 2)

    def dp_of(x_, m_, core_):
        return (x_ * 2 + m_) * 2 + core_

    def x_at(k):
        return lax.rem(x + k, 4)

    partner = (dp_of(x, m, 1 - core), tn)
    right = (dp_of(x_at(1), m, core), tn)
    left = (dp_of(x_at(3), m, core), tn)
    flip_dp = dp_of(x, 1 - m, core)
    zpeer = (flip_dp, tn)

    barrier = pltpu.get_barrier_semaphore()
    peers = []
    for k in (2, 1, 3, 0):
        if k:
            peers.append((dp, lax.rem(y + k, 4) * 2 + h))
        peers.append((dp, lax.rem(y + k, 4) * 2 + 1 - h))
        peers.append((flip_dp, lax.rem(y + k, 4) * 2 + 1 - h))
    peers += [zpeer, left, right, partner]
    for peer in peers:
        pl.semaphore_signal(barrier, inc=1, device_id=peer, device_id_type=MESH)

    order = [x_at(2), x_at(1), x_at(3), x]
    cot_ld = [
        pltpu.make_async_copy(cot_t.at[pl.ds(lo, n)], cot.at[pl.ds(pl.multiple_of(lo + 64 * h, 64), n)], cot_sem.at[k])
        for k, (lo, n) in enumerate(((0, 192), (192, 2176)))
    ]
    acts_ld = [pltpu.make_async_copy(acts.at[:, pl.ds(pl.multiple_of(p * 896, LANES), 896)], stage.at[k % 2], ld_sem.at[k])
               for k, p in enumerate(order)]
    st_ld = [pltpu.make_async_copy(hess, h_in, st_sem.at[0]), pltpu.make_async_copy(mom, m_in, st_sem.at[1])]
    acts_ld[0].start()
    cot_ld[0].start()
    acts_ld[1].start()

    cot[pl.ds(pl.multiple_of((1 - h) * 2368, 64), 64), :] = jnp.zeros((64, 1024), jnp.bfloat16)

    def remote(src, dst, ssem, rsem, dev):
        return pltpu.make_async_remote_copy(src_ref=src, dst_ref=dst, send_sem=ssem, recv_sem=rsem,
                                            device_id=dev, device_id_type=MESH)

    def tile_of(n, h_):
        return jnp.where(n == HALF, (NT - 1) * (1 - h_), n + h_ - (n > HALF).astype(jnp.int32))

    def matmul(rows, n):
        return lax.dot_general(
            rows, cot[pl.ds(pl.multiple_of(tile_of(n, h) * LANES, LANES), LANES), :],
            (((1,), (1,)), ((), ())), preferred_element_type=jnp.float32)

    def product(which, n):
        return matmul(acts_t[which].reshape(1792, 1024), n).reshape(4, 448, LANES)

    def q_of_x(n):
        return n + jnp.minimum(lax.div(jnp.maximum(n - 2, 0), 4), NZ)

    def q_of_z(i):
        return 5 * i + 6

    def d0_copy(k):
        return remote(d_send.at[0, order[k]], d_recv.at[0, order[k]], d0_ssem.at[k], d0_rsem.at[k], partner)

    def d_copy(q):
        return remote(d_send.at[lax.rem(q, 2)], d_recv.at[lax.rem(q, ND)], d_ssem.at[lax.rem(q, 2)],
                      d_rsem.at[lax.rem(q, ND)], partner)

    def x_set(at, half_of, far_, direct_, relay_, ssem, fsem, dsem, rsem):
        return (
            remote(half_of(at(2), 0), far_.at[0], ssem.at[0], fsem.at[0], left),
            remote(half_of(at(2), 1), far_.at[1], ssem.at[1], fsem.at[1], right),
            remote(half_of(at(1), 0), direct_.at[0], ssem.at[2], dsem.at[0], right),
            remote(half_of(at(3), 1), direct_.at[1], ssem.at[3], dsem.at[1], left),
            remote(half_of(at(3), 0), relay_.at[0], ssem.at[4], rsem.at[0], left),
            remote(half_of(at(1), 1), relay_.at[1], ssem.at[5], rsem.at[1], right),
        )

    def blk(n, k, half):
        return s_buf.at[lax.rem(n, NS), x_at(k), half]

    def x_copies(n):
        return x_set(lambda k: s_buf.at[lax.rem(n, NS), x_at(k)], lambda r, half: r.at[half],
                     far.at[n], direct.at[n], relay.at[n], x_ssem.at[lax.rem(n, NS)],
                     far_sem.at[n], direct_sem.at[n], relay_sem.at[n])

    def half_copies():
        short = pl.ds(0, 112)
        return x_set(lambda k: s_buf.at[HALF % NS, x_at(k)], lambda r, half: r.at[half, short, :],
                     far.at[HALF, :, short, :], direct.at[HALF, :, short, :], relay.at[HALF, :, short, :],
                     x_ssem.at[HALF % NS], far_sem.at[HALF], direct_sem.at[HALF], relay_sem.at[HALF])

    def zblk(i, k, half):
        return zs.at[i, x_at(k), m, pl.ds(112 * half, 112), :]

    def xz_copies(i):
        return x_set(lambda k: zs.at[i, x_at(k), m], lambda r, half: r.at[pl.ds(112 * half, 112), :],
                     far_z.at[i], direct_z.at[i], relay_z.at[i], xz_ssem.at[i],
                     far_sem.at[NX + i], direct_sem.at[NX + i], relay_sem.at[NX + i])

    def zf_copy(i, k):
        return remote(zs.at[i, k, 1 - m], zf.at[i, k], zf_ssem.at[i, k], zf_rsem.at[i, k], zpeer)

    def z_copies(n):
        s = lax.rem(n, NQ)
        return (remote(q_buf.at[s, 1 - m, h], z_recv.at[n, 0], z_ssem.at[s, 0], z_rsem.at[n, 0], zpeer),
                remote(q_buf.at[s, m, 1 - h], z_recv.at[n, 1], z_ssem.at[s, 1], z_rsem.at[n, 1], zpeer))

    def window(to):
        return pl.ds(pl.multiple_of(28 * to - 4 * lax.rem(to, 2), 8), WIN)

    def a_copies(n):
        s = lax.rem(n, NQ)
        out = []
        for k in (2, 1, 3):
            to = lax.rem(y + k, 4)
            out.append(remote(a_send.at[s, 0, window(to), :], g_buf.at[tn, n], a_ssem.at[s, k - 1], a_rsem.at[n], (dp, to * 2 + h)))
        for k in (2, 1, 3, 0):
            to = lax.rem(y + k, 4)
            out.append(remote(a_send.at[s, 1, window(to), :], g_buf.at[tn, n], a_ssem.at[s, 3 + k], a_rsem.at[n], (flip_dp, to * 2 + 1 - h)))
        return out

    def az_copies(i):
        out = []
        far_first = ((2, 1), (1, 1), (3, 1), (2, 0), (0, 1), (1, 0), (3, 0))
        for slot, (dy, dh) in enumerate(far_first):
            to_y, to_h = lax.rem(y + dy, 4), lax.rem(h + dh, 2)
            out.append(remote(az.at[i, to_h, window(to_y), :], g_buf.at[tn, NX + i],
                              az_ssem.at[i, slot], a_rsem.at[NX + i], (dp, to_y * 2 + to_h)))
        return out

    def h_copies(n):
        s = lax.rem(n, NH)
        out = []
        for k in range(1, 8):
            to = lax.rem(tn + k, 8)
            out.append(remote(hm_send.at[s, :, lax.div(to, 2), pl.ds(pl.multiple_of(24 * lax.rem(to, 2), 8), WIN), :],
                              hm_buf.at[tn, n], h_ssem.at[s, k - 1], h_rsem.at[n], (dp, to)))
        return out

    def turn(k):
        for i in range(7):
            block = stage[k % 2, :, i * LANES:(i + 1) * LANES].T
            done = 0
            while done < LANES:
                which, inside = divmod(i * LANES + done, 224)
                size = min(224 - inside, LANES - done)
                dest = (which // 2) * 224 + inside
                acts_t[which % 2, order[k], dest:dest + size, :] = block[done:done + size]
                done += size

    def own_piece(k):
        p = order[k]
        own = matmul(acts_t[core, p], jnp.int32(0))
        d0_copy(k).wait_recv()
        s_buf[0, p] = (own + d_recv[0, p]).reshape(2, 224, LANES)

    first = x_copies(0)
    for k in range(4):
        acts_ld[k].wait()
        turn(k)
        if k < 2:
            acts_ld[k + 2].start()
        if k == 0:
            cot_ld[1].start()
            cot_ld[0].wait()
        if k == 1:
            st_ld[0].start()
            st_ld[1].start()
        d_send[0, order[k]] = matmul(acts_t[1 - core, order[k]], jnp.int32(0))
        if k == 0:
            pl.semaphore_wait(barrier, len(peers))
        d0_copy(k).start()
        if k == 1:
            own_piece(0)
            first[0].start()
            first[1].start()
        if k == 2:
            own_piece(1)
            first[2].start()
    own_piece(2)
    first[3].start()
    own_piece(3)
    pl.semaphore_signal(d_free, inc=1, device_id=partner, device_id_type=MESH)

    def pass_on(cs, at_half, far_):
        for half, at in ((0, 3), (1, 1)):
            cs[half].wait_recv()
            b = at_half(at, half)
            b[...] = b[...] + far_[half]
            cs[4 + half].start()

    def send_partial(n, q):
        @pl.when(q >= 3)
        def _():
            d_copy(q - 2).wait_send()
        d_send[lax.rem(q, 2)] = product(1 - core, n)

        @pl.when(q >= ND)
        def _():
            pl.semaphore_wait(d_free, 1)
        d_copy(q).start()

    cot_ld[1].wait()
    send_partial(jnp.int32(1), jnp.int32(1))
    pass_on(first, lambda k, half: blk(0, k, half), far.at[0])
    for k in range(4):
        d0_copy(k).wait_send()
    st_ld[0].wait()
    st_ld[1].wait()
    for k, ref in enumerate((h_in, m_in)):
        tail[k] = jnp.concatenate([ref[:, 2304:], jnp.zeros((224, 64), jnp.float32)], axis=1)

    correction_power = jnp.float32(1.0)
    count = steps[0]
    for bit in range(15):
        correction_power = jnp.where(lax.rem(lax.div(count, 2 ** bit), 2) == 1,
                                     correction_power * jnp.float32(0.99 ** (2 ** bit)), correction_power)
    correction = 1.0 - correction_power
    factor = correction / gamma_table[layer[0]]
    y_odd = lax.rem(y, 2) == 1

    def trim(v, odd):
        return jnp.where(odd, v[4:], v[:28])

    def finish(tile, g, hs, mo):
        g, hs, mo = trim(g, y_odd), trim(hs, h == 1), trim(mo, h == 1)
        new = 0.99 * hs + (0.01 / TOKENS) * (g * g)
        fresh[pl.ds(tile, 28, stride=148), :] = new
        ratio[pl.ds(tile, 28, stride=148), :] = jnp.clip(mo * factor / new, -1.0, 1.0)

    lane = lax.broadcasted_iota(jnp.int32, (224, LANES), 1)

    def state_tile(k, ref, n):
        at = lambda i: ref[:, pl.ds(pl.multiple_of(i * LANES, LANES), LANES)]
        here = jnp.where(n < NT - 1, at(jnp.minimum(n, NT - 2)), tail[k])
        before = jnp.where(n > 0, at(jnp.maximum(n - 1, 0)), 0.0)
        moved = jnp.where(lane < 64, pltpu.roll(before, 64, 1), pltpu.roll(here, 64, 1))
        return jnp.where(h == 0, here, moved)

    low = lane[:112] < 64

    def pack(v):
        a, b = v[:112], v[112:]
        return jnp.where(h == 0, a + pltpu.roll(b, 64, 1), pltpu.roll(a, 64, 1) + b)

    def unpack(v):
        w = pltpu.roll(v, 64, 1)
        a = jnp.where(h == 0, jnp.where(low, v, 0.0), jnp.where(low, 0.0, w))
        b = jnp.where(h == 0, jnp.where(low, w, 0.0), jnp.where(low, 0.0, v))
        return jnp.concatenate([a, b], axis=0)

    def states_before(t):
        n = jnp.where(t <= 3, 3 * t - 3, jnp.where(t <= 5, 2 * t, t + 5))
        return jnp.minimum(n, NT)

    def state_step(n, carry):
        s = lax.rem(n, NH)

        @pl.when(n >= NH)
        def _():
            for c in h_copies(n - NH):
                c.wait_send()
        hm_send[s, 0] = state_tile(0, h_in, tile_of(n, h)).reshape(4, 56, LANES)
        hm_send[s, 1] = state_tile(1, m_in, tile_of(n, h)).reshape(4, 56, LANES)
        hm_buf[tn, n] = hm_send[s, :, y, pl.ds(pl.multiple_of(24 * h, 8), WIN), :]
        for c in h_copies(n):
            c.start()
        return carry

    def by_z_hi(dst, v):
        for y_ in range(4):
            for z_ in range(2):
                dst[z_, 28 * y_:28 * y_ + 28, :] = v[56 * y_ + 28 * z_:56 * y_ + 28 * z_ + 28]

    def own_sum(n, q):
        own = product(core, n)
        d_copy(q).wait_recv()
        total = (own + d_recv[lax.rem(q, ND)]).reshape(4, 2, 224, LANES)

        return total

    def free(q):
        @pl.when(q < NT - ND)
        def _():
            pl.semaphore_signal(d_free, inc=1, device_id=partner, device_id_type=MESH)

    def within(n, lo, hi):
        return pl.when(jnp.logical_and(n >= lo, n < hi))

    def body(t, carry):
        @within(t, 1, NX)
        def _():
            q = q_of_x(t)

            @pl.when(t >= NS)
            def _():
                for c in x_copies(t - NS):
                    c.wait_send()

            @pl.when(t < HALF)
            def _():
                s_buf[lax.rem(t, NS)] = own_sum(t, q)
                for c in x_copies(t)[:4]:
                    c.start()

            @pl.when(t == HALF)
            def _():
                total = own_sum(t, q)
                for k in range(4):
                    for half in range(2):
                        s_buf[HALF % NS, k, half, pl.ds(0, 112), :] = pack(total[k, half])
                for c in half_copies()[:4]:
                    c.start()
            free(q)

        @pl.when(t + 1 < NX)
        def _():
            send_partial(t + 1, q_of_x(t + 1))

        zi = lax.div(t - 5, 4)

        @pl.when(jnp.logical_and(lax.rem(t, 4) == 1, jnp.logical_and(t >= 5, t <= 4 * NZ + 1)))
        def _():
            q = q_of_z(zi)
            zs[zi] = own_sum(NX + zi, q)
            free(q)

        @within(t, 5, 5 + 4 * NZ)
        def _():
            zf_copy(zi, lax.rem(t - 5 + x + 2, 4)).start()

        @within(t, NX, NT)
        def _():
            i = t - NX
            cs = xz_copies(i)
            for k, go in ((2, (0, 1)), (1, (2,)), (3, (3,)), (0, ())):
                zf_copy(i, x_at(k)).wait_recv()
                zs[i, x_at(k), m] = zs[i, x_at(k), m] + zf[i, x_at(k)]
                for g in go:
                    cs[g].start()

        u2 = t - 1

        @within(u2, 1, HALF)
        def _():
            pass_on(x_copies(u2), lambda k, half: blk(u2, k, half), far.at[u2])

        @pl.when(u2 == HALF)
        def _():
            short = pl.ds(0, 112)
            pass_on(half_copies(), lambda k, half: s_buf.at[HALF % NS, x_at(k), half, short, :], far.at[HALF, :, short, :])

        @within(u2, NX, NT)
        def _():
            i = u2 - NX
            pass_on(xz_copies(i), lambda k, half: zblk(i, k, half), far_z.at[i])

        @pl.when(jnp.logical_and(lax.rem(t, 4) == 0, jnp.logical_and(t >= 4, t <= 4 * NZ)))
        def _():
            send_partial(NX + lax.div(t - 4, 4), q_of_z(lax.div(t - 4, 4)))

        lax.fori_loop(states_before(t), states_before(t + 1), state_step, 0)

        u3 = t - 3

        @within(u3, 0, NX)
        def _():
            @pl.when(u3 >= NQ)
            def _():
                for c in z_copies(u3 - NQ):
                    c.wait_send()
            s = lax.rem(u3, NQ)

            @pl.when(u3 < HALF)
            def _():
                cs = x_copies(u3)
                for half in range(2):
                    cs[2 + half].wait_recv()
                    cs[4 + half].wait_recv()
                    by_z_hi(q_buf.at[s, half], blk(u3, 0, half)[...] + direct[u3, half] + relay[u3, half])

            @pl.when(u3 == HALF)
            def _():
                cs = half_copies()
                for half in range(2):
                    cs[2 + half].wait_recv()
                    cs[4 + half].wait_recv()
                    total = s_buf[HALF % NS, x, half, :112] + direct[HALF, half, :112] + relay[HALF, half, :112]
                    by_z_hi(q_buf.at[s, half], unpack(total))
            for c in z_copies(u3):
                c.start()

        @within(u3, NX, NT)
        def _():
            i = u3 - NX
            cs = xz_copies(i)
            halves = []
            for half in range(2):
                cs[2 + half].wait_recv()
                cs[4 + half].wait_recv()
                halves.append(zblk(i, 0, half)[...] + direct_z[i, half] + relay_z[i, half])
            by_z_hi(az.at[i], jnp.concatenate(halves, axis=0))
            g_buf[tn, NX + i] = az[i, h, window(y), :]
            for c in az_copies(i):
                c.start()

        u4 = t - 6

        @within(u4, 0, NX)
        def _():
            s = lax.rem(u4, NQ)

            @pl.when(u4 >= NQ)
            def _():
                for c in a_copies(u4 - NQ):
                    c.wait_send()
            for c in z_copies(u4):
                c.wait_recv()
            a_send[s, 0] = q_buf[s, m, h] + z_recv[u4, 0]
            a_send[s, 1] = q_buf[s, 1 - m, 1 - h] + z_recv[u4, 1]
            g_buf[tn, u4] = a_send[s, 0, window(y), :]
            for c in a_copies(u4):
                c.start()

        u5 = t - 9

        @pl.when(u5 >= 0)
        def _():
            remote(g_buf.at[pl.ds(0, 7), u5], g_buf.at[pl.ds(0, 7), u5], a_ssem.at[0, 0], a_rsem.at[u5], partner).wait_recv()
            remote(hm_buf.at[pl.ds(0, 7), u5], hm_buf.at[pl.ds(0, 7), u5], h_ssem.at[0, 0], h_rsem.at[u5], partner).wait_recv()

            @pl.when(u5 != HALF)
            def _():
                for j in range(8):
                    finish(37 * (j // 2) + 18 * (j % 2) + tile_of(u5, j % 2), g_buf[j, u5], hm_buf[j, u5, 0], hm_buf[j, u5, 1])

            @pl.when(u5 == HALF)
            def _():
                for j in range(0, 8, 2):
                    finish(37 * (j // 2) + 18, *(a + b for a, b in (
                        (g_buf[j, HALF], g_buf[j + 1, HALF]),
                        (hm_buf[j, HALF, 0], hm_buf[j + 1, HALF, 0]), (hm_buf[j, HALF, 1], hm_buf[j + 1, HALF, 1]))))
        return carry

    lax.fori_loop(1, NT + 9, body, 0)

    for n in range(NX - NS, NX):
        for c in half_copies() if n == HALF else x_copies(n):
            c.wait_send()
    for n in range(NX - NQ, NX):
        for c in z_copies(n) + tuple(a_copies(n)):
            c.wait_send()
    for n in range(NT - NH, NT):
        for c in h_copies(n):
            c.wait_send()
    for i in range(NZ):
        for k in range(4):
            zf_copy(i, k).wait_send()
        for c in xz_copies(i) + tuple(az_copies(i)):
            c.wait_send()
    for q in range(NT - 2, NT):
        d_copy(q).wait_send()


def local(acts, cot, hess, mom, gamma_table, layer, steps):
    f32, bf16 = jnp.float32, jnp.bfloat16
    dma, vmem = pltpu.SemaphoreType.DMA, pltpu.VMEM
    anyspec = pl.BlockSpec(memory_space=pl.ANY)
    smem = pl.BlockSpec(memory_space=pltpu.SMEM)
    out = pltpu.VMEM((4144, LANES), f32)
    fresh, ratio = pl.pallas_call(
        kernel,
        out_shape=(out, out),
        in_specs=[anyspec] * 4 + [smem] * 3,
        out_specs=(pl.BlockSpec(memory_space=pltpu.VMEM),) * 2,
        scratch_shapes=[
            vmem((2, 4, 448, 1024), bf16), vmem((2, 1024, 896), bf16), vmem((NT * LANES, 1024), bf16),
            vmem((224, 2368), f32), vmem((224, 2368), f32), vmem((2, 224, LANES), f32),
            vmem((2, 4, 448, LANES), f32), vmem((ND, 4, 448, LANES), f32), vmem((NS, 4, 2, 224, LANES), f32),
            vmem((NX, 2, 224, LANES), f32), vmem((NX, 2, 224, LANES), f32), vmem((NX, 2, 224, LANES), f32),
            vmem((NQ, 2, 2, 112, LANES), f32), vmem((NX, 2, 112, LANES), f32), vmem((NQ, 2, 112, LANES), f32),
            vmem((8, NT, WIN, LANES), f32), vmem((NH, 2, 4, 56, LANES), f32), vmem((8, NT, 2, WIN, LANES), f32),
            vmem((NZ, 4, 2, 224, LANES), f32), vmem((NZ, 4, 224, LANES), f32),
            vmem((NZ, 2, 112, LANES), f32), vmem((NZ, 2, 112, LANES), f32), vmem((NZ, 2, 112, LANES), f32),
            vmem((NZ, 2, 112, LANES), f32),
            dma((4,)), dma((2,)), dma((2,)),
            dma((4,)), dma((4,)), dma((2,)), dma((ND,)), pltpu.SemaphoreType.REGULAR,
            dma((NS, 6)), dma((NT, 2)), dma((NT, 2)), dma((NT, 2)),
            dma((NQ, 2)), dma((NX, 2)), dma((NQ, 7)), dma((NT,)), dma((NH, 7)), dma((NT,)),
            dma((NZ, 4)), dma((NZ, 4)), dma((NZ, 6)), dma((NZ, 7)),
        ],
        compiler_params=pltpu.CompilerParams(collective_id=0, has_side_effects=True, vmem_limit_bytes=62500000),
    )(acts, cot.T, hess, mom, gamma_table, layer, steps)
    return fresh.reshape(-1), ratio.reshape(-1)


def solution(mesh):
    return jax.shard_map(
        local, mesh=mesh,
        in_specs=(P("dp", None), P("dp", "tensor"), P("dp", "tensor"), P("dp", "tensor"), P(None), P(None), P(None)),
        out_specs=(P(("dp", "tensor")), P(("dp", "tensor"))),
        check_vma=False)
```
